32 devices in a mesh: lat: 8 (over y, x, core), chan: 4 (over z).
Axes of the slice: x: 2, y: 2, z: 4, core: 2. Of those that a mesh axis runs over, the one named last changes fastest.
Arguments:
- field: bfloat16 [40, 642, 544], P('lat', None, 'chan'), may hold values from -6 to 6
- cotangent: bfloat16 [40, 642, 1024], P('lat'), may hold values from -6 to 6
- weight: bfloat16 [544, 1024], P('chan'), may hold values from -0.25 to 0.25
- lon_counts: int32 [40], P('lat'), may hold values from 20 to 5136, as said below
- point_mask: int32 [40, 5136], P('lat', 'chan'), may hold values 0 or 1
Outputs:
- field_grad: bfloat16 [40, 642, 544], P('lat', None, 'chan')
- weight_grad: float32 [1024, 544], P('lat', 'chan')
The draws below stay inside these ranges and needn't reach their ends.
Inputs may be any that keep to these rules, and one draw needn't show every extreme that they name: `lon_counts`: number of longitudes in use in a row; points from there to the end of the row are padding.
All inputs are finite; a program needn't handle non-finite values. No bound on the sum of `point_mask` on one device may be relied on, other than what follows from the above.
Results may differ from the reference program's by a relative error of at most 0.001.
Values sent between devices are 32-bit elements; how exact they have to be, the bound alone decides.
A program may use at most 64 MiB of HBM per device.

```python
import jax
import jax.numpy as jnp
from jax import lax

E = 1024
P_SIZE = 8
LON = 5136
C = 68
PATCHES = 642
ROWS = 40


def draw_lon_counts(key, part):
    row_index = jnp.arange(ROWS, dtype=jnp.int32)
    spread = max(1280 // ROWS, 1)
    latitude = row_index * 1280 // ROWS + jax.random.randint(key, (ROWS,), 0, spread, dtype=jnp.int32)
    latitude = jnp.minimum(latitude, 1279)
    latitude = jnp.where(row_index == ROWS - 1, 1279, latitude)
    latitude = jnp.where(row_index == 0, 0, latitude)
    return (20 + (LON - 20) * latitude // 1279).astype(jnp.int32)


def plant(values, own_key, least, largest):
    dims = values.shape
    place = [jax.random.randint(jax.random.fold_in(own_key, axis), (), 0, dims[axis]) for axis in range(len(dims))]
    values = values.at[tuple(place)].set(least)
    longest = dims.index(max(dims))
    place[longest] = (place[longest] + 1) % dims[longest]
    return values.at[tuple(place)].set(largest)


def strengthened(array, own_key, source, target, shards_of, factor):
    owner, partner = [(jnp.arange(array.shape[axis_at]) // (array.shape[axis_at] // shards_of)).reshape([-1 if axis == axis_at else 1 for axis in range(array.ndim)]) for axis_at in (source, target)]
    chosen = jax.random.permutation(own_key, shards_of)[partner]
    strong = (owner == chosen) | (owner == (partner + shards_of // 2) % shards_of)
    return jnp.where(strong, factor * array, array)


def steps_of(key, shape, split, low, top_value):
    loudness, own = 1.0, jax.random.fold_in(key, 6)
    for dim, parts in split:
        steps = jnp.exp(jax.random.uniform(jax.random.fold_in(own, dim), (parts,), jnp.float32, low / len(split), top_value / len(split)))
        loudness = loudness * jnp.repeat(steps, shape[dim] // parts).reshape([-1 if axis == dim else 1 for axis in range(len(shape))])
    return loudness


def centred(own_key, dims, width, bound, split=(), held_as=jnp.bfloat16):
    entries = jax.random.normal(own_key, dims, jnp.float32) * width
    if len(split) > 0:
        entries = steps_of(own_key, dims, split, -0.22, 0.18) * entries
    return jnp.clip(entries, min=-bound, max=bound).astype(held_as)


def heavy_noise(stream_key, shape, deviation, most, cuts, heavy, kind=jnp.bfloat16):
    drawn = deviation * jax.random.normal(stream_key, shape, jnp.float32)
    if cuts:
        drawn = drawn * steps_of(stream_key, shape, cuts, -0.22, 0.18)
    return jnp.clip(strengthened(drawn, jax.random.fold_in(stream_key, 3), *heavy), -most, most).astype(kind)


def setup_inputs(seed: int = 0) -> dict:
    splits = jax.random.split(jax.random.key(seed), 6)
    return {
        "field": centred(splits[0], (ROWS, PATCHES, C * P_SIZE), 1.0, 6.0, ((0, 8), (2, 4))),
        "cotangent": heavy_noise(splits[1], (ROWS, PATCHES, E), 1.0, 6.0, ((0, 8),), (0, 2, 8, 2.0)),
        "weight": centred(splits[2], (C * P_SIZE, E), (C * P_SIZE) ** -0.5, 0.25, ((0, 4),)),
        "lon_counts": draw_lon_counts(jax.random.fold_in(splits[5], 71), 0),
        "point_mask": plant((jax.random.randint(splits[4], (ROWS, LON), 0, 4) < 3).astype(jnp.int32), jax.random.fold_in(splits[4], 1), 0, 1),
    }


def reference(field, cotangent, weight, lon_counts, point_mask):
    positions = lax.broadcasted_iota(jnp.int32, point_mask.shape, 1)
    valid = jnp.where(positions < lon_counts[:, None], point_mask, 0)
    total = jnp.sum(valid).astype(jnp.float32)
    scale = lax.rsqrt(jnp.maximum(total, 1.0))
    point_valid = valid.reshape(ROWS, PATCHES, 1, P_SIZE)
    masked = (field.reshape(ROWS, PATCHES, C, P_SIZE) * point_valid.astype(jnp.bfloat16)).reshape(ROWS * PATCHES, C * P_SIZE)
    grads = cotangent.reshape(ROWS * PATCHES, E)
    product = lax.dot_general(grads, weight, (((1,), (1,)), ((), ())), preferred_element_type=jnp.float32)
    field_grad = (product.reshape(ROWS, PATCHES, C, P_SIZE) * point_valid.astype(jnp.float32)).reshape(ROWS, PATCHES, C * P_SIZE).astype(jnp.bfloat16)
    weight_grad = lax.dot_general(grads, masked, (((0,), (0,)), ((), ())), preferred_element_type=jnp.float32) * scale
    return (field_grad, weight_grad)
```

```python
import functools

import jax
import jax.numpy as jnp
from jax import lax
from jax.experimental import pallas as pl
from jax.experimental.pallas import tpu as pltpu
from jax.sharding import PartitionSpec as P

P_SIZE = 8
LANES = 128
MESH = pl.DeviceIdType.MESH


def round_up(value, multiple):
    return (value + multiple - 1) // multiple * multiple


def kernel(
    n_lat, n_chan,
    field_hbm, cot_hbm, weight_hbm, lon_ref, mask_hbm,
    grad_ref, wgrad_ref,
    cot, field, weight, masks, expand, spread, masked,
    part, pair_recv, chip_sum, chip_recv, count_send, count_recv,
    cot_sem, load_sem, mask_send, mask_recv, count_ssem, count_rsem,
    pair_ssem, pair_rsem, chip_ssem, chip_rsem,
):
    rows, features, patches = field.shape
    width = masks.shape[2]
    n_chips = n_lat // 2
    owned = wgrad_ref.shape[1]
    lat, chan = lax.axis_index("lat"), lax.axis_index("chan")
    chip, core = lat // 2, lax.rem(lat, 2)
    partner = chip * 2 + 1 - core

    load_mask = pltpu.make_async_copy(mask_hbm, masks.at[chan], load_sem.at[0])
    load_mask.start()
    load_weight = pltpu.make_async_copy(weight_hbm, weight, load_sem.at[1])
    load_weight.start()
    for r in range(rows):
        pltpu.make_async_copy(cot_hbm.at[r], cot.at[r], cot_sem.at[r]).start()
    load_field = pltpu.make_async_copy(field_hbm, field, load_sem.at[2])
    load_field.start()

    barrier = pltpu.get_barrier_semaphore()
    for o in range(1, n_chan):
        pl.semaphore_signal(barrier, inc=1, device_id=(lat, lax.rem(chan + o, n_chan)), device_id_type=MESH)
    for o in range(1, n_lat):
        pl.semaphore_signal(barrier, inc=1, device_id=(lax.rem(lat + o, n_lat), chan), device_id_type=MESH)

    lane_of = lax.broadcasted_iota(jnp.int32, spread.shape[1:], 0)
    patch_of = lax.broadcasted_iota(jnp.int32, spread.shape[1:], 1)
    shifts = sorted({z * width % P_SIZE for z in range(n_chan)})
    for index, shift in enumerate(shifts):
        spread[index] = jnp.where((lane_of + shift) // P_SIZE == patch_of, 1.0, 0.0).astype(jnp.bfloat16)

    load_mask.wait()
    pl.semaphore_wait(barrier, n_chan + n_lat - 2)
    mask_copies = []
    for o in range(1, n_chan):
        copy = pltpu.make_async_remote_copy(
            src_ref=masks.at[chan], dst_ref=masks.at[chan],
            send_sem=mask_send.at[o - 1], recv_sem=mask_recv.at[o - 1],
            device_id=(lat, lax.rem(chan + o, n_chan)), device_id_type=MESH,
        )
        copy.start()
        mask_copies.append(copy)

    load_weight.wait()

    @pl.loop(0, rows)
    def _(r):
        pltpu.make_async_copy(cot_hbm.at[r], cot.at[r], cot_sem.at[r]).wait()
        grad_ref[r] = lax.dot_general(
            weight[...], cot[r], (((1,), (1,)), ((), ())), preferred_element_type=jnp.float32
        ).astype(jnp.bfloat16)

    for copy in mask_copies:
        copy.wait()

    padded = expand.shape[1]
    lane = lax.broadcasted_iota(jnp.int32, (P_SIZE, width), 1)
    sub = lax.broadcasted_iota(jnp.int32, (P_SIZE, width), 0)
    counts = jnp.zeros((1, width), jnp.int32)
    valid_all = jnp.zeros((rows * P_SIZE, padded), jnp.float32)
    for z in range(n_chan):
        first, shift = z * width // P_SIZE, z * width % P_SIZE
        pick = lax.rem(lane + shift, P_SIZE) == sub
        position = lane[:1] + z * width
        block = masks[z]
        placed = []
        for r in range(rows):
            valid = jnp.where(position < lon_ref[r], block[r:r + 1], 0)
            counts = counts + valid
            placed.append(jnp.where(pick, jnp.broadcast_to(valid, (P_SIZE, width)), 0))
        left = jnp.concatenate(placed, axis=0).astype(jnp.float32).astype(jnp.bfloat16)
        local = jnp.dot(left, spread[shifts.index(shift)], preferred_element_type=jnp.float32)
        if padded > local.shape[1]:
            local = jnp.concatenate(
                [local, jnp.zeros((rows * P_SIZE, padded - local.shape[1]), jnp.float32)], axis=1
            )
        valid_all = valid_all + (pltpu.roll(local, first, axis=1) if first else local)
    expand[...] = valid_all
    total_here = jnp.sum(counts)
    count_send[...] = jnp.full(count_send.shape, total_here, jnp.int32)

    load_field.wait()
    for r in range(rows):
        valid8 = expand[r * P_SIZE:(r + 1) * P_SIZE, :patches]
        tiled = jnp.concatenate([valid8] * (features // P_SIZE), axis=0).astype(jnp.bfloat16)
        masked[r] = field[r] * tiled
        grad_ref[r] = grad_ref[r] * tiled

    count_copies = []
    for o in range(1, n_lat):
        copy = pltpu.make_async_remote_copy(
            src_ref=count_send, dst_ref=count_recv.at[o - 1],
            send_sem=count_ssem.at[o - 1], recv_sem=count_rsem.at[o - 1],
            device_id=(lax.rem(lat + o, n_lat), chan), device_id_type=MESH,
        )
        copy.start()
        count_copies.append(copy)

    def pair_copy(s):
        return pltpu.make_async_remote_copy(
            src_ref=part.at[1 - core, s], dst_ref=pair_recv.at[s],
            send_sem=pair_ssem.at[s], recv_sem=pair_rsem.at[s],
            device_id=(partner, chan), device_id_type=MESH,
        )

    def chip_copy(s):
        return pltpu.make_async_remote_copy(
            src_ref=chip_sum.at[s], dst_ref=chip_recv.at[s],
            send_sem=chip_ssem.at[s], recv_sem=chip_rsem.at[s],
            device_id=(lax.rem(chip + s + 1, n_chips) * 2 + core, chan), device_id_type=MESH,
        )

    def forward(s):
        pair_copy(s).wait()
        chip_sum[s] = part[core, s] + pair_recv[s]
        chip_copy(s).start()

    for s in range(n_chips):
        owner = lax.rem(chip + s + 1, n_chips)
        columns = pl.ds(pl.multiple_of(owner * (2 * owned), 2 * owned), 2 * owned)
        chunk = jnp.zeros((features, 2 * owned), jnp.float32)
        for r in range(rows):
            chunk = chunk + jnp.dot(masked[r], cot[r, :, columns], preferred_element_type=jnp.float32)
        part[0, s] = chunk[:, :owned]
        part[1, s] = chunk[:, owned:]
        pair_copy(s).start()
        if s >= 1:
            forward(s - 1)

    last = n_chips - 1
    total = count_send[...]
    for o in range(1, n_lat):
        count_copies[o - 1].wait()
        total = total + count_recv[o - 1]
    scale = lax.rsqrt(jnp.maximum(total.astype(jnp.float32), 1.0))[:1]
    pair_copy(last).wait()
    summed = part[core, last] + pair_recv[last]
    for s in range(n_chips - 1):
        chip_copy(s).wait()
        summed = summed + chip_recv[s]
    wgrad_ref[...] = summed * jnp.broadcast_to(scale[:, :1], summed.shape)


def fused(n_lat, n_chan, field, cotangent, weight, lon_counts, point_mask):
    rows, patches, features = field.shape
    width = point_mask.shape[1]
    embed = cotangent.shape[2]
    owned = embed // n_lat
    n_chips = n_lat // 2
    shifts = len({z * width % P_SIZE for z in range(n_chan)})
    covered = round_up(width // P_SIZE + 2, LANES)
    padded = max(round_up(patches, LANES), covered)
    anywhere = pl.BlockSpec(memory_space=pl.ANY)
    vmem = pl.BlockSpec(memory_space=pltpu.VMEM)
    dma = pltpu.SemaphoreType.DMA
    grad, wgrad = pl.pallas_call(
        functools.partial(kernel, n_lat, n_chan),
        out_shape=(
            jax.ShapeDtypeStruct((rows, features, patches), jnp.bfloat16),
            jax.ShapeDtypeStruct((features, owned), jnp.float32),
        ),
        in_specs=[anywhere, anywhere, anywhere, pl.BlockSpec(memory_space=pltpu.SMEM), anywhere],
        out_specs=(vmem, vmem),
        scratch_shapes=[
            pltpu.VMEM((rows, patches, embed), jnp.bfloat16),
            pltpu.VMEM((rows, features, patches), jnp.bfloat16),
            pltpu.VMEM((features, embed), jnp.bfloat16),
            pltpu.VMEM((n_chan, rows, width), jnp.int32),
            pltpu.VMEM((rows * P_SIZE, padded), jnp.float32),
            pltpu.VMEM((shifts, width, covered), jnp.bfloat16),
            pltpu.VMEM((rows, features, patches), jnp.bfloat16),
            pltpu.VMEM((2, n_chips, features, owned), jnp.float32),
            pltpu.VMEM((n_chips, features, owned), jnp.float32),
            pltpu.VMEM((n_chips - 1, features, owned), jnp.float32),
            pltpu.VMEM((n_chips - 1, features, owned), jnp.float32),
            pltpu.VMEM((8, LANES), jnp.int32),
            pltpu.VMEM((n_lat - 1, 8, LANES), jnp.int32),
            dma((rows,)),
            dma((3,)),
            dma((n_chan - 1,)),
            dma((n_chan - 1,)),
            dma((n_lat - 1,)),
            dma((n_lat - 1,)),
            dma((n_chips,)),
            dma((n_chips,)),
            dma((n_chips - 1,)),
            dma((n_chips - 1,)),
        ],
        compiler_params=pltpu.CompilerParams(
            collective_id=0, has_side_effects=True, vmem_limit_bytes=61 * 1024 * 1024
        ),
    )(jnp.swapaxes(field, 1, 2), cotangent, weight, lon_counts, point_mask)
    return jnp.swapaxes(grad, 1, 2), wgrad.T


def plain(field, cotangent, weight, lon_counts, point_mask):
    row_count, patch_count, features = field.shape
    channels = features // P_SIZE
    full_mask = lax.all_gather(point_mask, "chan", axis=1, tiled=True)
    positions = lax.broadcasted_iota(jnp.int32, full_mask.shape, 1)
    valid = jnp.where(positions < lon_counts[:, None], full_mask, 0)
    total = lax.psum(jnp.sum(valid), "lat")
    scale = lax.rsqrt(jnp.maximum(total.astype(jnp.float32), 1.0))
    point_valid = valid.reshape(row_count, patch_count, 1, P_SIZE)
    masked = (
        field.reshape(row_count, patch_count, channels, P_SIZE) * point_valid.astype(jnp.bfloat16)
    ).reshape(row_count, patch_count, features)
    outcome = lax.dot_general(
        cotangent, weight, (((2,), (1,)), ((), ())), preferred_element_type=jnp.float32
    )
    field_grad = (
        (
            outcome.reshape(row_count, patch_count, channels, P_SIZE)
            * point_valid.astype(jnp.float32)
        )
        .reshape(row_count, patch_count, features)
        .astype(jnp.bfloat16)
    )
    summed = lax.dot_general(
        cotangent, masked, (((0, 1), (0, 1)), ((), ())), preferred_element_type=jnp.float32
    )
    weight_grad = lax.psum_scatter(summed * scale, "lat", scatter_dimension=0, tiled=True)
    return (field_grad, weight_grad)


def solution(mesh):
    n_lat, n_chan = mesh.shape["lat"], mesh.shape["chan"]

    def local(field, cotangent, weight, lon_counts, point_mask):
        whole_tiles = cotangent.shape[2] % (n_lat * LANES) == 0
        if n_lat % 2 == 0 and n_lat > 2 and n_chan > 1 and whole_tiles:
            return fused(n_lat, n_chan, field, cotangent, weight, lon_counts, point_mask)
        return plain(field, cotangent, weight, lon_counts, point_mask)

    in_specs = (
        P("lat", None, "chan"),
        P("lat", None, None),
        P("chan", None),
        P("lat"),
        P("lat", "chan"),
    )
    out_specs = (P("lat", None, "chan"), P("lat", "chan"))
    return jax.shard_map(local, mesh=mesh, in_specs=in_specs, out_specs=out_specs, check_vma=False)
```

```python
import functools

import jax
import jax.numpy as jnp
from jax import lax
from jax.experimental import pallas as pl
from jax.experimental.pallas import tpu as pltpu
from jax.sharding import PartitionSpec as P

P_SIZE = 8
LANES = 128
MESH = pl.DeviceIdType.MESH


def round_up(value, multiple):
    return (value + multiple - 1) // multiple * multiple


def kernel(
    n_lat, n_chan,
    field_hbm, cot_hbm, weight_hbm, lon_hbm, mask_hbm,
    grad_ref, wgrad_ref,
    cot, field, weight, lon_ref, masks, expand, spread, masked, tiled,
    part, pair_recv, chip_sum, chip_recv, count_send, count_recv,
    cot_sem, load_sem, mask_send, mask_recv, count_ssem, count_rsem,
    pair_ssem, pair_rsem, chip_ssem, chip_rsem,
):
    rows, features, patches = field.shape
    width = masks.shape[2]
    n_chips = n_lat // 2
    owned = wgrad_ref.shape[1]
    lat, chan = lax.axis_index("lat"), lax.axis_index("chan")
    chip, core = lat // 2, lax.rem(lat, 2)
    partner = chip * 2 + 1 - core

    load_mask = pltpu.make_async_copy(mask_hbm, masks.at[chan], load_sem.at[0])
    load_mask.start()
    load_lon = pltpu.make_async_copy(lon_hbm, lon_ref, load_sem.at[3])
    load_lon.start()
    load_weight = pltpu.make_async_copy(weight_hbm, weight, load_sem.at[1])
    load_weight.start()
    for r in range(rows):
        pltpu.make_async_copy(cot_hbm.at[r], cot.at[r], cot_sem.at[r]).start()
    load_field = pltpu.make_async_copy(field_hbm, field, load_sem.at[2])
    load_field.start()

    barrier = pltpu.get_barrier_semaphore()
    for o in range(1, n_chan):
        pl.semaphore_signal(barrier, inc=1, device_id=(lat, lax.rem(chan + o, n_chan)), device_id_type=MESH)
    for o in range(1, n_lat):
        pl.semaphore_signal(barrier, inc=1, device_id=(lax.rem(lat + o, n_lat), chan), device_id_type=MESH)

    lane_of = lax.broadcasted_iota(jnp.int32, spread.shape[1:], 0)
    patch_of = lax.broadcasted_iota(jnp.int32, spread.shape[1:], 1)
    shifts = sorted({z * width % P_SIZE for z in range(n_chan)})
    for index, shift in enumerate(shifts):
        spread[index] = jnp.where((lane_of + shift) // P_SIZE == patch_of, 1.0, 0.0).astype(jnp.bfloat16)

    load_mask.wait()
    pl.semaphore_wait(barrier, n_chan + n_lat - 2)
    mask_copies = []
    for o in range(1, n_chan):
        copy = pltpu.make_async_remote_copy(
            src_ref=masks.at[chan], dst_ref=masks.at[chan],
            send_sem=mask_send.at[o - 1], recv_sem=mask_recv.at[o - 1],
            device_id=(lat, lax.rem(chan + o, n_chan)), device_id_type=MESH,
        )
        copy.start()
        mask_copies.append(copy)

    load_weight.wait()

    early = rows - 2 if rows > 2 else rows

    def product(r):
        return lax.dot_general(
            weight[...], cot[r], (((1,), (1,)), ((), ())), preferred_element_type=jnp.float32
        ).astype(jnp.bfloat16)

    @pl.loop(0, early)
    def _(r):
        pltpu.make_async_copy(cot_hbm.at[r], cot.at[r], cot_sem.at[r]).wait()
        grad_ref[r] = product(r)

    load_lon.wait()
    for copy in mask_copies:
        copy.wait()

    padded = expand.shape[1]
    lane = lax.broadcasted_iota(jnp.int32, (P_SIZE, width), 1)
    sub = lax.broadcasted_iota(jnp.int32, (P_SIZE, width), 0)
    counts = jnp.zeros((1, width), jnp.int32)
    valid_all = jnp.zeros((rows * P_SIZE, padded), jnp.float32)
    for z in range(n_chan):
        first, shift = z * width // P_SIZE, z * width % P_SIZE
        pick = lax.rem(lane + shift, P_SIZE) == sub
        position = lane[:1] + z * width
        block = masks[z]
        placed = []
        for r in range(rows):
            valid = jnp.where(position < lon_ref[r], block[r:r + 1], 0)
            counts = counts + valid
            placed.append(jnp.where(pick, jnp.broadcast_to(valid, (P_SIZE, width)), 0))
        left = jnp.concatenate(placed, axis=0).astype(jnp.float32).astype(jnp.bfloat16)
        local = jnp.dot(left, spread[shifts.index(shift)], preferred_element_type=jnp.float32)
        if padded > local.shape[1]:
            local = jnp.concatenate(
                [local, jnp.zeros((rows * P_SIZE, padded - local.shape[1]), jnp.float32)], axis=1
            )
        valid_all = valid_all + (pltpu.roll(local, first, axis=1) if first else local)
    expand[...] = valid_all
    total_here = jnp.sum(counts)
    count_send[...] = jnp.full(count_send.shape, total_here, jnp.int32)

    load_field.wait()
    for r in range(rows):
        valid8 = expand[r * P_SIZE:(r + 1) * P_SIZE, :patches]
        tiled[r] = jnp.concatenate([valid8] * (features // P_SIZE), axis=0).astype(jnp.bfloat16)
        masked[r] = field[r] * tiled[r]
    for r in range(early, rows):
        pltpu.make_async_copy(cot_hbm.at[r], cot.at[r], cot_sem.at[r]).wait()

    count_copies = []
    for o in range(1, n_lat):
        copy = pltpu.make_async_remote_copy(
            src_ref=count_send, dst_ref=count_recv.at[o - 1],
            send_sem=count_ssem.at[o - 1], recv_sem=count_rsem.at[o - 1],
            device_id=(lax.rem(lat + o, n_lat), chan), device_id_type=MESH,
        )
        copy.start()
        count_copies.append(copy)

    def pair_copy(s):
        return pltpu.make_async_remote_copy(
            src_ref=part.at[1 - core, s], dst_ref=pair_recv.at[s],
            send_sem=pair_ssem.at[s], recv_sem=pair_rsem.at[s],
            device_id=(partner, chan), device_id_type=MESH,
        )

    def chip_copy(s):
        return pltpu.make_async_remote_copy(
            src_ref=chip_sum.at[s], dst_ref=chip_recv.at[s],
            send_sem=chip_ssem.at[s], recv_sem=chip_rsem.at[s],
            device_id=(lax.rem(chip + s + 1, n_chips) * 2 + core, chan), device_id_type=MESH,
        )

    def forward(s):
        pair_copy(s).wait()
        chip_sum[s] = part[core, s] + pair_recv[s]
        chip_copy(s).start()

    for s in range(n_chips):
        owner = lax.rem(chip + s + 1, n_chips)
        columns = pl.ds(pl.multiple_of(owner * (2 * owned), 2 * owned), 2 * owned)
        chunk = jnp.zeros((features, 2 * owned), jnp.float32)
        for r in range(rows):
            chunk = chunk + jnp.dot(masked[r], cot[r, :, columns], preferred_element_type=jnp.float32)
        part[0, s] = chunk[:, :owned]
        part[1, s] = chunk[:, owned:]
        pair_copy(s).start()
        if s >= 1:
            forward(s - 1)

    @pl.loop(early, rows)
    def _(r):
        grad_ref[r] = product(r) * tiled[r]

    @pl.loop(0, early)
    def _(r):
        grad_ref[r] = grad_ref[r] * tiled[r]

    last = n_chips - 1
    total = count_send[...]
    for o in range(1, n_lat):
        count_copies[o - 1].wait()
        total = total + count_recv[o - 1]
    scale = lax.rsqrt(jnp.maximum(total.astype(jnp.float32), 1.0))[:1]
    pair_copy(last).wait()
    summed = part[core, last] + pair_recv[last]
    for s in range(n_chips - 1):
        chip_copy(s).wait()
        summed = summed + chip_recv[s]
    wgrad_ref[...] = summed * jnp.broadcast_to(scale[:, :1], summed.shape)


def write_out(grad_ref, wgrad_ref, grad_hbm, wgrad_hbm, sem):
    copies = [
        pltpu.make_async_copy(grad_ref, grad_hbm, sem.at[0]),
        pltpu.make_async_copy(wgrad_ref, wgrad_hbm, sem.at[1]),
    ]
    for copy in copies:
        copy.start()
    for copy in copies:
        copy.wait()


def fused(n_lat, n_chan, field, cotangent, weight, lon_counts, point_mask):
    rows, patches, features = field.shape
    width = point_mask.shape[1]
    embed = cotangent.shape[2]
    owned = embed // n_lat
    n_chips = n_lat // 2
    shifts = len({z * width % P_SIZE for z in range(n_chan)})
    covered = round_up(width // P_SIZE + 2, LANES)
    padded = max(round_up(patches, LANES), covered)
    anywhere = pl.BlockSpec(memory_space=pltpu.HBM)
    vmem = pl.BlockSpec(memory_space=pltpu.VMEM)
    dma = pltpu.SemaphoreType.DMA
    grad, wgrad = pl.pallas_call(
        functools.partial(kernel, n_lat, n_chan),
        out_shape=(
            jax.ShapeDtypeStruct((rows, features, patches), jnp.bfloat16),
            jax.ShapeDtypeStruct((features, owned), jnp.float32),
        ),
        in_specs=[anywhere] * 5,
        out_specs=(vmem, vmem),
        scratch_shapes=[
            pltpu.VMEM((rows, patches, embed), jnp.bfloat16),
            pltpu.VMEM((rows, features, patches), jnp.bfloat16),
            pltpu.VMEM((features, embed), jnp.bfloat16),
            pltpu.SMEM((rows,), jnp.int32),
            pltpu.VMEM((n_chan, rows, width), jnp.int32),
            pltpu.VMEM((rows * P_SIZE, padded), jnp.float32),
            pltpu.VMEM((shifts, width, covered), jnp.bfloat16),
            pltpu.VMEM((rows, features, patches), jnp.bfloat16),
            pltpu.VMEM((rows, features, patches), jnp.bfloat16),
            pltpu.VMEM((2, n_chips, features, owned), jnp.float32),
            pltpu.VMEM((n_chips, features, owned), jnp.float32),
            pltpu.VMEM((n_chips - 1, features, owned), jnp.float32),
            pltpu.VMEM((n_chips - 1, features, owned), jnp.float32),
            pltpu.VMEM((8, LANES), jnp.int32),
            pltpu.VMEM((n_lat - 1, 8, LANES), jnp.int32),
            dma((rows,)),
            dma((4,)),
            dma((n_chan - 1,)),
            dma((n_chan - 1,)),
            dma((n_lat - 1,)),
            dma((n_lat - 1,)),
            dma((n_chips,)),
            dma((n_chips,)),
            dma((n_chips - 1,)),
            dma((n_chips - 1,)),
        ],
        compiler_params=pltpu.CompilerParams(
            collective_id=0, has_side_effects=True, vmem_limit_bytes=24 * 1024 * 1024
        ),
    )(
        pltpu.with_memory_space_constraint(jnp.swapaxes(field, 1, 2), pltpu.HBM),
        pltpu.with_memory_space_constraint(cotangent, pltpu.HBM),
        pltpu.with_memory_space_constraint(weight, pltpu.HBM),
        pltpu.with_memory_space_constraint(lon_counts, pltpu.HBM),
        pltpu.with_memory_space_constraint(point_mask, pltpu.HBM),
    )
    grad, wgrad = pl.pallas_call(
        write_out,
        out_shape=(
            jax.ShapeDtypeStruct(grad.shape, grad.dtype),
            jax.ShapeDtypeStruct(wgrad.shape, wgrad.dtype),
        ),
        in_specs=[vmem, vmem],
        out_specs=(anywhere, anywhere),
        scratch_shapes=[dma((2,))],
        compiler_params=pltpu.CompilerParams(vmem_limit_bytes=4 * 1024 * 1024),
    )(grad, wgrad)
    return jnp.swapaxes(grad, 1, 2), wgrad.T


def plain(field, cotangent, weight, lon_counts, point_mask):
    row_count, patch_count, features = field.shape
    channels = features // P_SIZE
    full_mask = lax.all_gather(point_mask, "chan", axis=1, tiled=True)
    positions = lax.broadcasted_iota(jnp.int32, full_mask.shape, 1)
    valid = jnp.where(positions < lon_counts[:, None], full_mask, 0)
    total = lax.psum(jnp.sum(valid), "lat")
    scale = lax.rsqrt(jnp.maximum(total.astype(jnp.float32), 1.0))
    point_valid = valid.reshape(row_count, patch_count, 1, P_SIZE)
    masked = (
        field.reshape(row_count, patch_count, channels, P_SIZE) * point_valid.astype(jnp.bfloat16)
    ).reshape(row_count, patch_count, features)
    outcome = lax.dot_general(
        cotangent, weight, (((2,), (1,)), ((), ())), preferred_element_type=jnp.float32
    )
    field_grad = (
        (
            outcome.reshape(row_count, patch_count, channels, P_SIZE)
            * point_valid.astype(jnp.float32)
        )
        .reshape(row_count, patch_count, features)
        .astype(jnp.bfloat16)
    )
    summed = lax.dot_general(
        cotangent, masked, (((0, 1), (0, 1)), ((), ())), preferred_element_type=jnp.float32
    )
    weight_grad = lax.psum_scatter(summed * scale, "lat", scatter_dimension=0, tiled=True)
    return (field_grad, weight_grad)


def solution(mesh):
    n_lat, n_chan = mesh.shape["lat"], mesh.shape["chan"]

    def local(field, cotangent, weight, lon_counts, point_mask):
        whole_tiles = cotangent.shape[2] % (n_lat * LANES) == 0
        if n_lat % 2 == 0 and n_lat > 2 and n_chan > 1 and whole_tiles:
            return fused(n_lat, n_chan, field, cotangent, weight, lon_counts, point_mask)
        return plain(field, cotangent, weight, lon_counts, point_mask)

    in_specs = (
        P("lat", None, "chan"),
        P("lat", None, None),
        P("chan", None),
        P("lat"),
        P("lat", "chan"),
    )
    out_specs = (P("lat", None, "chan"), P("lat", "chan"))
    return jax.shard_map(local, mesh=mesh, in_specs=in_specs, out_specs=out_specs, check_vma=False)
```

```python
import functools

import jax
import jax.numpy as jnp
from jax import lax
from jax.experimental import pallas as pl
from jax.experimental.pallas import tpu as pltpu
from jax.sharding import PartitionSpec as P

P_SIZE = 8
LANES = 128
MESH = pl.DeviceIdType.MESH


def round_up(value, multiple):
    return (value + multiple - 1) // multiple * multiple


def flip(index, bits):
    result, bit = index, 1
    while bit <= bits:
        if bits & bit:
            result = result + bit * (1 - 2 * lax.rem(lax.div(index, bit), 2))
        bit *= 2
    return result


def kernel(
    n_lat, n_chan,
    field_hbm, cot_hbm, weight_hbm, lon_hbm, mask_hbm,
    grad_ref, wgrad_ref,
    cot, field, weight, lon_ref, masks, expand, spread, masked, tiled,
    part, pair_recv, chip_sum, chip_recv, count_send, count_recv,
    cot_sem, load_sem, mask_send, mask_recv, count_ssem, count_rsem,
    pair_ssem, pair_rsem, chip_ssem, chip_rsem,
):
    rows, features, patches = field.shape
    width = masks.shape[2]
    n_chips = n_lat // 2
    owned = wgrad_ref.shape[1]
    lat, chan = lax.axis_index("lat"), lax.axis_index("chan")
    chip, core = lax.div(lat, 2), lax.rem(lat, 2)
    partner = flip(lat, 1)

    load_mask = pltpu.make_async_copy(mask_hbm, masks.at[chan], load_sem.at[0])
    load_mask.start()
    load_lon = pltpu.make_async_copy(lon_hbm, lon_ref, load_sem.at[3])
    load_lon.start()
    load_weight = pltpu.make_async_copy(weight_hbm, weight, load_sem.at[1])
    load_weight.start()
    for r in range(rows):
        pltpu.make_async_copy(cot_hbm.at[r], cot.at[r], cot_sem.at[r]).start()
    load_field = pltpu.make_async_copy(field_hbm, field, load_sem.at[2])
    load_field.start()

    barrier = pltpu.get_barrier_semaphore()
    for o in range(1, n_chan):
        pl.semaphore_signal(barrier, inc=1, device_id=(lat, flip(chan, o)), device_id_type=MESH)
    for o in range(1, n_lat):
        pl.semaphore_signal(barrier, inc=1, device_id=(flip(lat, o), chan), device_id_type=MESH)

    lane_of = lax.broadcasted_iota(jnp.int32, spread.shape[1:], 0)
    patch_of = lax.broadcasted_iota(jnp.int32, spread.shape[1:], 1)
    shifts = sorted({z * width % P_SIZE for z in range(n_chan)})
    for index, shift in enumerate(shifts):
        spread[index] = jnp.where((lane_of + shift) // P_SIZE == patch_of, 1.0, 0.0).astype(jnp.bfloat16)

    load_mask.wait()
    pl.semaphore_wait(barrier, n_chan + n_lat - 2)
    mask_copies = {}
    for o in reversed(range(1, n_chan)):
        copy = pltpu.make_async_remote_copy(
            src_ref=masks.at[chan], dst_ref=masks.at[chan],
            send_sem=mask_send.at[o - 1], recv_sem=mask_recv.at[o - 1],
            device_id=(lat, flip(chan, o)), device_id_type=MESH,
        )
        copy.start()
        mask_copies[o] = copy

    load_weight.wait()

    early = rows - 2 if rows > 2 else rows

    def product(r):
        return lax.dot_general(
            weight[...], cot[r], (((1,), (1,)), ((), ())), preferred_element_type=jnp.float32
        ).astype(jnp.bfloat16)

    @pl.loop(0, early)
    def _(r):
        pltpu.make_async_copy(cot_hbm.at[r], cot.at[r], cot_sem.at[r]).wait()
        grad_ref[r] = product(r)

    load_lon.wait()
    padded = expand.shape[1]
    lane = lax.broadcasted_iota(jnp.int32, (P_SIZE, width), 1)
    sub = lax.broadcasted_iota(jnp.int32, (P_SIZE, width), 0)
    counts = jnp.zeros((1, width), jnp.int32)
    valid_all = jnp.zeros((rows * P_SIZE, padded), jnp.float32)
    for o in range(n_chan):
        if o > 0:
            mask_copies[o].wait_recv()
        z = flip(chan, o)
        first, shift = lax.div(z * width, P_SIZE), lax.rem(z * width, P_SIZE)
        kind = sum((z == other).astype(jnp.int32) * shifts.index(other * width % P_SIZE) for other in range(n_chan))
        pick = lax.rem(lane + shift, P_SIZE) == sub
        position = lane[:1] + z * width
        placed = []
        for r in range(rows):
            valid = jnp.where(position < lon_ref[r], masks[z, r:r + 1], 0)
            counts = counts + valid
            placed.append(jnp.where(pick, jnp.broadcast_to(valid, (P_SIZE, width)), 0))
        left = jnp.concatenate(placed, axis=0).astype(jnp.float32).astype(jnp.bfloat16)
        local = jnp.dot(left, spread[kind], preferred_element_type=jnp.float32)
        if padded > local.shape[1]:
            local = jnp.concatenate(
                [local, jnp.zeros((rows * P_SIZE, padded - local.shape[1]), jnp.float32)], axis=1
            )
        valid_all = valid_all + pltpu.roll(local, first, axis=1)
    expand[...] = valid_all
    total_here = jnp.sum(counts)
    count_send[...] = jnp.full(count_send.shape, total_here, jnp.int32)

    load_field.wait()
    for r in range(rows):
        valid8 = expand[r * P_SIZE:(r + 1) * P_SIZE, :patches]
        tiled[r] = jnp.concatenate([valid8] * (features // P_SIZE), axis=0).astype(jnp.bfloat16)
        masked[r] = field[r] * tiled[r]
    for r in range(early, rows):
        pltpu.make_async_copy(cot_hbm.at[r], cot.at[r], cot_sem.at[r]).wait()

    count_copies = []
    for o in range(1, n_lat):
        copy = pltpu.make_async_remote_copy(
            src_ref=count_send, dst_ref=count_recv.at[o - 1],
            send_sem=count_ssem.at[o - 1], recv_sem=count_rsem.at[o - 1],
            device_id=(flip(lat, o), chan), device_id_type=MESH,
        )
        copy.start()
        count_copies.append(copy)

    def pair_copy(s):
        return pltpu.make_async_remote_copy(
            src_ref=part.at[1 - core, s], dst_ref=pair_recv.at[s],
            send_sem=pair_ssem.at[s], recv_sem=pair_rsem.at[s],
            device_id=(partner, chan), device_id_type=MESH,
        )

    def chip_copy(s):
        return pltpu.make_async_remote_copy(
            src_ref=chip_sum.at[s], dst_ref=chip_recv.at[s],
            send_sem=chip_ssem.at[s], recv_sem=chip_rsem.at[s],
            device_id=(flip(chip, n_chips - 1 - s) * 2 + core, chan), device_id_type=MESH,
        )

    def forward(s):
        pair_copy(s).wait_recv()
        chip_sum[s] = part[core, s] + pair_recv[s]
        chip_copy(s).start()

    for s in range(n_chips):
        owner = flip(chip, n_chips - 1 - s)
        columns = pl.ds(pl.multiple_of(owner * (2 * owned), 2 * owned), 2 * owned)
        chunk = jnp.zeros((features, 2 * owned), jnp.float32)
        for r in range(rows):
            chunk = chunk + jnp.dot(masked[r], cot[r, :, columns], preferred_element_type=jnp.float32)
        part[0, s] = chunk[:, :owned]
        part[1, s] = chunk[:, owned:]
        pair_copy(s).start()
        if s == n_chips - 2:
            forward(0)
    for s in range(1, n_chips - 1):
        forward(s)

    @pl.loop(early, rows)
    def _(r):
        grad_ref[r] = product(r) * tiled[r]

    @pl.loop(0, early)
    def _(r):
        grad_ref[r] = grad_ref[r] * tiled[r]

    last = n_chips - 1
    total = count_send[...]
    for o in range(1, n_lat):
        count_copies[o - 1].wait()
        total = total + count_recv[o - 1]
    scale = lax.rsqrt(jnp.maximum(total.astype(jnp.float32), 1.0))[:1]
    for s in range(last):
        pair_copy(s).wait_send()
    for o in range(1, n_chan):
        mask_copies[o].wait_send()
    pair_copy(last).wait()
    summed = part[core, last] + pair_recv[last]
    for s in range(n_chips - 1):
        chip_copy(s).wait()
        summed = summed + chip_recv[s]
    wgrad_ref[...] = summed * jnp.broadcast_to(scale[:, :1], summed.shape)


def write_out(grad_ref, wgrad_ref, grad_hbm, wgrad_hbm, sem):
    copies = [
        pltpu.make_async_copy(grad_ref, grad_hbm, sem.at[0]),
        pltpu.make_async_copy(wgrad_ref, wgrad_hbm, sem.at[1]),
    ]
    for copy in copies:
        copy.start()
    for copy in copies:
        copy.wait()


def fused(n_lat, n_chan, field, cotangent, weight, lon_counts, point_mask):
    rows, patches, features = field.shape
    width = point_mask.shape[1]
    embed = cotangent.shape[2]
    owned = embed // n_lat
    n_chips = n_lat // 2
    shifts = len({z * width % P_SIZE for z in range(n_chan)})
    covered = round_up(width // P_SIZE + 2, LANES)
    padded = max(round_up(patches, LANES), covered)
    anywhere = pl.BlockSpec(memory_space=pltpu.HBM)
    vmem = pl.BlockSpec(memory_space=pltpu.VMEM)
    dma = pltpu.SemaphoreType.DMA
    grad, wgrad = pl.pallas_call(
        functools.partial(kernel, n_lat, n_chan),
        out_shape=(
            jax.ShapeDtypeStruct((rows, features, patches), jnp.bfloat16),
            jax.ShapeDtypeStruct((features, owned), jnp.float32),
        ),
        in_specs=[anywhere] * 5,
        out_specs=(vmem, vmem),
        scratch_shapes=[
            pltpu.VMEM((rows, patches, embed), jnp.bfloat16),
            pltpu.VMEM((rows, features, patches), jnp.bfloat16),
            pltpu.VMEM((features, embed), jnp.bfloat16),
            pltpu.SMEM((rows,), jnp.int32),
            pltpu.VMEM((n_chan, rows, width), jnp.int32),
            pltpu.VMEM((rows * P_SIZE, padded), jnp.float32),
            pltpu.VMEM((shifts, width, covered), jnp.bfloat16),
            pltpu.VMEM((rows, features, patches), jnp.bfloat16),
            pltpu.VMEM((rows, features, patches), jnp.bfloat16),
            pltpu.VMEM((2, n_chips, features, owned), jnp.float32),
            pltpu.VMEM((n_chips, features, owned), jnp.float32),
            pltpu.VMEM((n_chips - 1, features, owned), jnp.float32),
            pltpu.VMEM((n_chips - 1, features, owned), jnp.float32),
            pltpu.VMEM((8, LANES), jnp.int32),
            pltpu.VMEM((n_lat - 1, 8, LANES), jnp.int32),
            dma((rows,)),
            dma((4,)),
            dma((n_chan - 1,)),
            dma((n_chan - 1,)),
            dma((n_lat - 1,)),
            dma((n_lat - 1,)),
            dma((n_chips,)),
            dma((n_chips,)),
            dma((n_chips - 1,)),
            dma((n_chips - 1,)),
        ],
        compiler_params=pltpu.CompilerParams(
            collective_id=0, has_side_effects=True, vmem_limit_bytes=24 * 1024 * 1024
        ),
    )(
        pltpu.with_memory_space_constraint(jnp.swapaxes(field, 1, 2), pltpu.HBM),
        pltpu.with_memory_space_constraint(cotangent, pltpu.HBM),
        pltpu.with_memory_space_constraint(weight, pltpu.HBM),
        pltpu.with_memory_space_constraint(lon_counts, pltpu.HBM),
        pltpu.with_memory_space_constraint(point_mask, pltpu.HBM),
    )
    grad, wgrad = pl.pallas_call(
        write_out,
        out_shape=(
            jax.ShapeDtypeStruct(grad.shape, grad.dtype),
            jax.ShapeDtypeStruct(wgrad.shape, wgrad.dtype),
        ),
        in_specs=[vmem, vmem],
        out_specs=(anywhere, anywhere),
        scratch_shapes=[dma((2,))],
        compiler_params=pltpu.CompilerParams(vmem_limit_bytes=4 * 1024 * 1024),
    )(grad, wgrad)
    return jnp.swapaxes(grad, 1, 2), wgrad.T


def plain(field, cotangent, weight, lon_counts, point_mask):
    row_count, patch_count, features = field.shape
    channels = features // P_SIZE
    full_mask = lax.all_gather(point_mask, "chan", axis=1, tiled=True)
    positions = lax.broadcasted_iota(jnp.int32, full_mask.shape, 1)
    valid = jnp.where(positions < lon_counts[:, None], full_mask, 0)
    total = lax.psum(jnp.sum(valid), "lat")
    scale = lax.rsqrt(jnp.maximum(total.astype(jnp.float32), 1.0))
    point_valid = valid.reshape(row_count, patch_count, 1, P_SIZE)
    masked = (
        field.reshape(row_count, patch_count, channels, P_SIZE) * point_valid.astype(jnp.bfloat16)
    ).reshape(row_count, patch_count, features)
    outcome = lax.dot_general(
        cotangent, weight, (((2,), (1,)), ((), ())), preferred_element_type=jnp.float32
    )
    field_grad = (
        (
            outcome.reshape(row_count, patch_count, channels, P_SIZE)
            * point_valid.astype(jnp.float32)
        )
        .reshape(row_count, patch_count, features)
        .astype(jnp.bfloat16)
    )
    summed = lax.dot_general(
        cotangent, masked, (((0, 1), (0, 1)), ((), ())), preferred_element_type=jnp.float32
    )
    weight_grad = lax.psum_scatter(summed * scale, "lat", scatter_dimension=0, tiled=True)
    return (field_grad, weight_grad)


def solution(mesh):
    n_lat, n_chan = mesh.shape["lat"], mesh.shape["chan"]

    def local(field, cotangent, weight, lon_counts, point_mask):
        whole_tiles = cotangent.shape[2] % (n_lat * LANES) == 0
        powers = n_lat & (n_lat - 1) == 0 and n_chan & (n_chan - 1) == 0
        if powers and n_lat > 2 and n_chan > 1 and whole_tiles:
            return fused(n_lat, n_chan, field, cotangent, weight, lon_counts, point_mask)
        return plain(field, cotangent, weight, lon_counts, point_mask)

    in_specs = (
        P("lat", None, "chan"),
        P("lat", None, None),
        P("chan", None),
        P("lat"),
        P("lat", "chan"),
    )
    out_specs = (P("lat", None, "chan"), P("lat", "chan"))
    return jax.shard_map(local, mesh=mesh, in_specs=in_specs, out_specs=out_specs, check_vma=False)
```
